32 devices in a mesh: member: 2 (over x), dp: 8 (over z, y), mp: 2 (over core).
Axes of the slice: x: 2, y: 2, z: 4, core: 2. Of those that a mesh axis runs over, the one named last changes fastest.
Arguments:
- activations: bfloat16 [2048, 2048], P(('member', 'dp')), parts along dimension 0, may hold values from -6 to 6
- out_grads: bfloat16 [2048, 10240], P(('member', 'dp'), 'mp'), parts along dimension 0, may hold values from -0.19921875 to 0.19921875
- slot_table: int32 [4, 16], P(('member', 'mp')), parts along dimension 0, may hold values from 0 to 15, each once within a row
- exponent_index: int32 [4, 16], P(('member', 'mp')), parts along dimension 0, may hold values from 0 to 1
- damping_index: int32 [4, 16], P(('member', 'mp')), parts along dimension 0, may hold values from 0 to 3
Outputs:
- update: bfloat16 [4096, 10240], P('member', 'mp'), parts along dimension 0
- preconditioners: bfloat16 [4, 16, 2, 1024, 1024], P(('member', 'mp'), 'dp'), parts along dimension 0
The draws below stay inside these ranges and needn't reach their ends.
There are 2 independent parts, one for each index of `member`. The reference program is written for one: setup_inputs(seed, part) draws one part's arguments, and reference() takes and returns one part's arrays. A program takes and returns all parts, laid end to end along the dimension named above; each array names one. Nothing has to cross between parts.
Inputs may be any that keep to these rules, and one draw needn't show every extreme that they name: `slot_table`: each row is a permutation of 0 to 15; slot s belongs to dp index s.
All inputs are finite; a program needn't handle non-finite values.
Results may differ from the reference program's by a relative error of at most 0.006.
The reference program's roundings to bfloat16 on the way (of `gradient`, `half_step` and `assembled`) count: a program that leaves them out, or rounds other values in their place, can miss the bound.
Values may be sent and summed in bfloat16 or wider, within the bound.
A program may use at most 192 MiB of HBM per device.

```python
import jax
import jax.numpy as jnp
from jax import lax

D_WIN = 2048
FF_WIN = 10240
BLK = 1024
SLOTS = 16
ITERS = 2
TOKENS = 1024
N_MP = 2


def plant(entries, stream_key, least, top_value):
    index_at = [jax.random.randint(jax.random.fold_in(stream_key, axis), (), 0, length) for axis, length in enumerate(entries.shape)]
    widest = entries.shape.index(max(entries.shape))
    neighbour = index_at[:widest] + [(index_at[widest] + 1) % entries.shape[widest]] + index_at[widest + 1:]
    return entries.at[tuple(index_at)].set(least).at[tuple(neighbour)].set(top_value)


def block_levels(own_key, dims, cuts, low, top_value):
    factor_of, own = 1.0, jax.random.fold_in(own_key, 6)
    for dim, shards_of in cuts:
        heights = jnp.exp(jax.random.uniform(jax.random.fold_in(own, dim), (shards_of,), jnp.float32, low / len(cuts), top_value / len(cuts)))
        factor_of = factor_of * jnp.repeat(heights, dims[dim] // shards_of).reshape([-1 if axis == dim else 1 for axis in range(len(dims))])
    return factor_of


def gaussian(key, extent, width, bound, split=(), kind=jnp.bfloat16):
    array = width * jax.random.normal(key, extent, jnp.float32)
    if split:
        array = array * block_levels(key, extent, split, -0.22, 0.18)
    return jnp.clip(array, -bound, bound).astype(kind)


def setup_inputs(seed: int = 0, part: int = 0) -> dict:
    keys = jax.random.split(jax.random.key(seed), 6)
    part_keys = jax.random.split(jax.random.fold_in(keys[5], part), 6)
    activations = gaussian(part_keys[0], (TOKENS, D_WIN), 1.0, 6.0, ((0, 8),))
    out_grads = gaussian(part_keys[1], (TOKENS, FF_WIN), 0.03125, 0.19921875, ((0, 8), (1, 2)))
    slot_table = jax.vmap(lambda own: jax.random.permutation(own, SLOTS))(jax.random.split(part_keys[2], N_MP)).reshape((N_MP, SLOTS)).astype(jnp.int32)
    exponent_index = plant(jax.random.randint(part_keys[3], (N_MP, SLOTS), 0, 2), jax.random.fold_in(part_keys[3], 1), 0, 1).astype(jnp.int32)
    damping_index = plant(jax.random.randint(part_keys[4], (N_MP, SLOTS), 0, 4), jax.random.fold_in(part_keys[4], 1), 0, 3).astype(jnp.int32)
    return dict(activations=activations, out_grads=out_grads, slot_table=slot_table, exponent_index=exponent_index, damping_index=damping_index)


ROOT_ORDERS = (2.0, 4.0)
DAMPINGS = (0.03, 0.1, 0.3, 1.0)

def table_value(picked, values_table):
    values = jnp.asarray(values_table, jnp.float32)
    matches = jnp.arange(len(values_table), dtype=jnp.int32) == picked
    return jnp.sum(jnp.where(matches, values, 0.0))

def half_dot(first, second):
    return jnp.dot(first.astype(jnp.bfloat16), second.astype(jnp.bfloat16), preferred_element_type=jnp.float32)

def inverse_root(statistic, root_order, quartic, damping):
    dimension = statistic.shape[0]
    identity = jnp.eye(dimension, dtype=jnp.float32)
    damped = statistic + damping * (jnp.trace(statistic) / dimension + 1.0) * identity
    current = damped * (dimension / (2.0 * jnp.trace(damped)))
    factor = ((root_order + 1.0) * identity - current) / root_order
    estimate = factor
    for sweep in range(1, ITERS):
        square = half_dot(factor, factor)
        fourth = half_dot(square, square)
        raised = jnp.where(quartic, fourth, square)
        current = half_dot(raised, current)
        factor = ((root_order + 1.0) * identity - current) / root_order
        estimate = half_dot(estimate, factor)
    return estimate.astype(jnp.bfloat16)

def precondition(act_block, grad_block, root_order, quartic, damping):
    gradient = lax.dot_general(act_block, grad_block, (((0,), (0,)), ((), ())), preferred_element_type=jnp.float32).astype(jnp.bfloat16)
    left_stat = lax.dot_general(gradient, gradient, (((1,), (1,)), ((), ())), preferred_element_type=jnp.float32)
    right_stat = lax.dot_general(gradient, gradient, (((0,), (0,)), ((), ())), preferred_element_type=jnp.float32)
    left_root = inverse_root(left_stat, root_order, quartic, damping)
    right_root = inverse_root(right_stat, root_order, quartic, damping)
    half_step = jnp.dot(left_root, gradient, preferred_element_type=jnp.float32).astype(jnp.bfloat16)
    block_update = jnp.dot(half_step, right_root, preferred_element_type=jnp.float32).astype(jnp.bfloat16)
    return (block_update, jnp.stack([left_root, right_root]))

def reference(activations, out_grads, slot_table, exponent_index, damping_index):
    row_blocks = D_WIN // BLK
    col_blocks = FF_WIN // (N_MP * BLK)
    half_blocks = row_blocks * col_blocks
    acts_grid = activations.reshape(TOKENS, row_blocks, BLK)
    grads_grid = out_grads.reshape(TOKENS, N_MP, col_blocks, BLK)
    flat_exp = exponent_index.reshape(N_MP * SLOTS)
    flat_damp = damping_index.reshape(N_MP * SLOTS)

    def one_slot(flat_slot):
        half_id = flat_slot // SLOTS
        slot_id = flat_slot % SLOTS
        exp_pick = lax.dynamic_index_in_dim(flat_exp, flat_slot, 0, keepdims=False)
        damp_pick = lax.dynamic_index_in_dim(flat_damp, flat_slot, 0, keepdims=False)
        root_order = table_value(exp_pick, ROOT_ORDERS)
        quartic = exp_pick == 1
        damping = table_value(damp_pick, DAMPINGS)
        table_row = lax.dynamic_index_in_dim(slot_table, half_id, 0, keepdims=False)[:half_blocks]
        matches = table_row == slot_id
        filled = jnp.any(matches)
        block_id = jnp.sum(jnp.where(matches, jnp.arange(half_blocks, dtype=jnp.int32), 0)).astype(jnp.int32)
        act_block = lax.dynamic_index_in_dim(acts_grid, block_id // col_blocks, 1, keepdims=False)
        grad_half = lax.dynamic_index_in_dim(grads_grid, half_id, 1, keepdims=False)
        grad_block = lax.dynamic_index_in_dim(grad_half, block_id % col_blocks, 1, keepdims=False)
        act_block = jnp.where(filled, act_block, jnp.zeros_like(act_block))
        grad_block = jnp.where(filled, grad_block, jnp.zeros_like(grad_block))
        return precondition(act_block, grad_block, root_order, quartic, damping)
    block_updates, roots = lax.map(one_slot, jnp.arange(N_MP * SLOTS, dtype=jnp.int32))
    by_slot = block_updates.reshape(N_MP, SLOTS, BLK, BLK)
    chosen = jnp.take_along_axis(by_slot, slot_table[:, :half_blocks][:, :, None, None], axis=1)
    assembled = chosen.reshape(N_MP, row_blocks, col_blocks, BLK, BLK).transpose(1, 3, 0, 2, 4).reshape(D_WIN, FF_WIN)
    wide = assembled.astype(jnp.float32)
    total_sq = jnp.sum(wide * wide)
    rescale = lax.rsqrt(total_sq / (D_WIN * FF_WIN) + 1.0)
    update = (wide * rescale).astype(jnp.bfloat16)
    return (update, roots.reshape(N_MP, SLOTS, 2, BLK, BLK))
```

```python
import functools

import jax
import jax.numpy as jnp
from jax import lax
from jax.experimental import pallas as pl
from jax.experimental.pallas import tpu as pltpu
from jax.sharding import PartitionSpec as P

BLK = 1024
TILE = 256

ROOT_ORDERS = (2.0, 4.0)
DAMPINGS = (0.03, 0.1, 0.3, 1.0)


NORMAL = (((1,), (0,)), ((), ()))
LEFT_T = (((0,), (0,)), ((), ()))
RIGHT_T = (((1,), (1,)), ((), ()))


def product(lhs, rhs, dims, finish):
    @pl.loop(0, BLK // TILE)
    def _(step):
        start = pl.multiple_of(step * TILE, TILE)
        rows = pl.ds(start, TILE)
        side = lhs[:, rows] if dims is LEFT_T else lhs[rows, :]
        finish(start, rows, lax.dot_general(side, rhs[...], dims, preferred_element_type=jnp.float32))


def on_diagonal(start):
    row = lax.broadcasted_iota(jnp.int32, (TILE, BLK), 0) + start
    return row == lax.broadcasted_iota(jnp.int32, (TILE, BLK), 1)


def fold(values):
    return jnp.sum((values * values).reshape(TILE // 8, 8, BLK), axis=0)


def block_kernel(with_update, ints, floats, act, grad, *refs):
    if with_update:
        update, square_sum, gradient, current, factor, second, powers, sums, roots = refs
    else:
        roots_out, gradient, current, factor, second, powers, sums = refs
        roots = roots_out.at[0]
    slot = pl.program_id(0)
    filled = ints[4 * slot + 2]
    quartic = ints[4 * slot + 3]
    damping = floats[slot]
    order = jnp.where(quartic == 1, 4.0, 2.0)
    inverse_order = jnp.where(quartic == 1, 0.25, 0.5)

    sums[...] = jnp.zeros_like(sums)

    def keep_gradient(start, rows, tile):
        rounded = jnp.where(filled == 1, tile, 0.0).astype(jnp.bfloat16)
        gradient[rows, :] = rounded
        sums[...] += fold(rounded.astype(jnp.float32))

    product(act, grad, LEFT_T, keep_gradient)
    trace = jnp.sum(sums[...])
    shift = damping * (trace / BLK + 1.0)
    scale = BLK / (2.0 * (trace + BLK * shift))

    for side, dims in ((0, RIGHT_T), (1, LEFT_T)):

        def start_root(start, rows, tile):
            diagonal = on_diagonal(start)
            value = (tile + jnp.where(diagonal, shift, 0.0)) * scale
            current[rows, :] = value.astype(jnp.bfloat16)
            factor[rows, :] = ((jnp.where(diagonal, order + 1.0, 0.0) - value) * inverse_order).astype(
                jnp.bfloat16
            )

        def keep_power(index):
            def finish(start, rows, tile):
                powers[index, rows, :] = tile.astype(jnp.bfloat16)

            return finish

        def next_factor(start, rows, tile):
            second[rows, :] = (
                (jnp.where(on_diagonal(start), order + 1.0, 0.0) - tile) * inverse_order
            ).astype(jnp.bfloat16)

        def keep_root(start, rows, tile):
            roots[side, rows, :] = tile.astype(jnp.bfloat16)

        product(gradient, gradient, dims, start_root)
        product(factor, factor, NORMAL, keep_power(0))

        @pl.when(quartic == 1)
        def _():
            product(powers.at[0], powers.at[0], NORMAL, keep_power(1))

        product(powers.at[quartic], current, NORMAL, next_factor)
        product(factor, second, NORMAL, keep_root)

    if with_update:

        def keep_half(start, rows, tile):
            current[rows, :] = tile.astype(jnp.bfloat16)

        def keep_update(start, rows, tile):
            rounded = tile.astype(jnp.bfloat16)
            update[0, rows, :] = rounded
            sums[...] += fold(rounded.astype(jnp.float32))

        product(roots.at[0], gradient, NORMAL, keep_half)
        sums[...] = jnp.zeros_like(sums)
        product(current, roots.at[1], NORMAL, keep_update)
        square_sum[0] = sums[...]


def run_blocks(with_update, inputs, act_blocks, row_ids, col_ids, filled, exponents, dampings):
    count = row_ids.shape[0]
    tokens = inputs.shape[0]
    ints = jnp.stack(
        [row_ids, col_ids + act_blocks, filled.astype(jnp.int32), exponents.astype(jnp.int32)], axis=1
    ).reshape(-1)
    square = pltpu.VMEM((BLK, BLK), jnp.bfloat16)
    scratch = [square, square, square, square, pltpu.VMEM((2, BLK, BLK), jnp.bfloat16), pltpu.VMEM((8, BLK), jnp.float32)]
    if with_update:
        scratch.append(pltpu.VMEM((2, BLK, BLK), jnp.bfloat16))
        shapes = (
            jax.ShapeDtypeStruct((count, BLK, BLK), jnp.bfloat16),
            jax.ShapeDtypeStruct((count, 8, BLK), jnp.float32),
        )
        specs = (
            pl.BlockSpec((1, BLK, BLK), lambda i, a, b: (i, 0, 0)),
            pl.BlockSpec((1, 8, BLK), lambda i, a, b: (i, 0, 0)),
        )
    else:
        shapes = jax.ShapeDtypeStruct((count, 2, BLK, BLK), jnp.bfloat16)
        specs = pl.BlockSpec((1, 2, BLK, BLK), lambda i, a, b: (i, 0, 0, 0))
    products = 13 if with_update else 11
    return pl.pallas_call(
        functools.partial(block_kernel, with_update),
        out_shape=shapes,
        grid_spec=pltpu.PrefetchScalarGridSpec(
            num_scalar_prefetch=2,
            grid=(count,),
            in_specs=[
                pl.BlockSpec((tokens, BLK), lambda i, a, b: (0, a[4 * i])),
                pl.BlockSpec((tokens, BLK), lambda i, a, b: (0, a[4 * i + 1])),
            ],
            out_specs=specs,
            scratch_shapes=scratch,
        ),
        compiler_params=pltpu.CompilerParams(vmem_limit_bytes=52 * 1024 * 1024),
        cost_estimate=pl.CostEstimate(
            flops=count * products * 2 * BLK**3, bytes_accessed=count * 8 * BLK**2, transcendentals=0
        ),
        name="block_update" if with_update else "block_roots",
    )(ints, jnp.stack([dampings[i] for i in range(count)]), inputs, inputs)


def ring_order(size):
    return list(range(0, size, 2)) + list(range(size - 1 - size % 2, 0, -2))


def two_way_ring(own, size, place):
    order = ring_order(size)
    forward = [(order[i], order[(i + 1) % size]) for i in range(size)]
    backward = [(b, a) for a, b in forward]
    order_array = jnp.array(order, jnp.int32)
    seat_array = jnp.array([order.index(i) for i in range(size)], jnp.int32)
    seat = seat_array[lax.axis_index("dp")]
    rows = own.shape[0]
    whole = (size - 1) // 2
    ahead = behind = own
    for step in range(1, whole + 1):
        ahead = lax.ppermute(ahead, "dp", forward)
        behind = lax.ppermute(behind, "dp", backward)
        place(order_array[(seat - step) % size], 0, ahead)
        place(order_array[(seat + step) % size], 0, behind)
    if size % 2 == 0:
        across = order_array[(seat + size // 2) % size]
        place(across, 0, lax.ppermute(ahead[: rows // 2], "dp", forward))
        place(across, rows // 2, lax.ppermute(behind[rows // 2 :], "dp", backward))


def on_device(activations, out_grads, slot_table, exponent_index, damping_index):
    tok_count = activations.shape[0]
    row_blocks = activations.shape[1] // BLK
    half_width = out_grads.shape[1]
    col_blocks = half_width // BLK
    half_blocks = row_blocks * col_blocks
    slot_count = slot_table.shape[1]
    owners = lax.axis_size("dp")
    halves = lax.axis_size("mp")
    per_owner = slot_count // owners
    me = lax.axis_index("dp")
    shared = min(owners, half_blocks)

    own = jnp.concatenate([activations, out_grads], axis=1)
    gathered = [lax.dynamic_update_slice(
        jnp.zeros((owners * tok_count, own.shape[1]), own.dtype), own, (me * tok_count, 0)
    )]

    def place_input(source, offset, piece):
        gathered[0] = lax.dynamic_update_slice(gathered[0], piece, (source * tok_count + offset, 0))

    two_way_ring(own, owners, place_input)
    inputs = gathered[0]

    table = slot_table[0]
    exponents = exponent_index[0]
    picks = damping_index[0]
    dampings = jnp.sum(
        jnp.where(
            picks[:, None] == jnp.arange(len(DAMPINGS), dtype=jnp.int32)[None, :],
            jnp.asarray(DAMPINGS, jnp.float32)[None, :],
            0.0,
        ),
        axis=1,
    )

    def blocks(ids):
        slots = table[ids]
        return run_blocks(
            True, inputs, row_blocks, ids // col_blocks, ids % col_blocks,
            jnp.ones_like(ids), exponents[slots], dampings[slots],
        )

    mine = (me % shared).astype(jnp.int32)
    first, first_sum = blocks(mine[None])
    total = jnp.where(me < shared, jnp.sum(first_sum), 0.0)
    extra_count = half_blocks - shared
    extras = []
    if extra_count:
        extra, extra_sum = blocks(jnp.arange(shared, half_blocks, dtype=jnp.int32))
        total = total + jnp.where(me == 0, jnp.sum(extra_sum), 0.0)
        extras = [extra[i] for i in range(extra_count)]
    total_sq = lax.psum(total, ("dp", "mp"))
    rescale = lax.rsqrt(total_sq / (row_blocks * BLK * half_width * halves) + 1.0)

    slots = me * per_owner + jnp.arange(per_owner, dtype=jnp.int32)
    matches = table[None, :half_blocks] == slots[:, None]
    filled = jnp.any(matches, axis=1)
    ids = jnp.sum(jnp.where(matches, jnp.arange(half_blocks, dtype=jnp.int32)[None, :], 0), axis=1)
    roots = run_blocks(
        False, inputs, row_blocks, ids // col_blocks, ids % col_blocks, filled,
        exponents[slots], dampings[slots],
    )

    canvas = [jnp.zeros((row_blocks * BLK, half_width), jnp.bfloat16)]

    def place_block(source, offset, piece):
        scaled = (piece.astype(jnp.float32) * rescale).astype(jnp.bfloat16)
        at = ((source // col_blocks) * BLK + offset, (source % col_blocks) * BLK)
        if shared < owners:
            before = lax.dynamic_slice(canvas[0], at, scaled.shape)
            scaled = jnp.where(source < shared, scaled, before)
        canvas[0] = lax.dynamic_update_slice(canvas[0], scaled, at)

    for position in range(extra_count):
        place_block(jnp.int32(shared + position), 0, extras[position])
    place_block(me, 0, first[0])
    two_way_ring(first[0], owners, place_block)
    return (canvas[0], roots[None])


def solution(mesh):
    placed = (
        P(("member", "dp"), None),
        P(("member", "dp"), "mp"),
        P(("member", "mp"), None),
        P(("member", "mp"), None),
        P(("member", "mp"), None),
    )
    return jax.shard_map(
        on_device,
        mesh=mesh,
        in_specs=placed,
        out_specs=(P("member", "mp"), P(("member", "mp"), "dp", None, None, None)),
        check_vma=False,
    )
```

```python
import functools

import jax
import jax.numpy as jnp
from jax import lax
from jax.experimental import pallas as pl
from jax.experimental.pallas import tpu as pltpu
from jax.sharding import PartitionSpec as P

BLK = 1024

ROOT_ORDERS = (2.0, 4.0)
DAMPINGS = (0.03, 0.1, 0.3, 1.0)


NORMAL = (((1,), (0,)), ((), ()))
LEFT_T = (((0,), (0,)), ((), ()))
RIGHT_T = (((1,), (1,)), ((), ()))


def product(lhs, rhs, dims, finish):
    finish(lax.dot_general(lhs[...], rhs[...], dims, preferred_element_type=jnp.float32))


def on_diagonal():
    row = lax.broadcasted_iota(jnp.int32, (BLK, BLK), 0)
    return row == lax.broadcasted_iota(jnp.int32, (BLK, BLK), 1)


def fold(values):
    return jnp.sum((values * values).reshape(BLK // 8, 8, BLK), axis=0)


def block_kernel(with_update, unread, ints, floats, act, grad, *refs):
    refs = refs[unread:]
    if with_update:
        update, square_sum, gradient, current, factor, second, square, roots = refs
    else:
        roots_out, gradient, current, factor, second, square = refs
        roots = roots_out.at[0]
    filled = ints[2]
    quartic = ints[3]
    damping = floats[0]
    order = jnp.where(quartic == 1, 4.0, 2.0)
    inverse_order = jnp.where(quartic == 1, 0.25, 0.5)

    tile = lax.dot_general(act[...], grad[...], LEFT_T, preferred_element_type=jnp.float32)
    rounded = jnp.where(filled == 1, tile, 0.0).astype(jnp.bfloat16)
    gradient[...] = rounded
    trace = jnp.sum(fold(rounded.astype(jnp.float32)))
    shift = damping * (trace / BLK + 1.0)
    scale = BLK / (2.0 * (trace + BLK * shift))

    for side, dims in ((0, RIGHT_T), (1, LEFT_T)):

        def start_root(tile):
            diagonal = on_diagonal()
            value = (tile + jnp.where(diagonal, shift, 0.0)) * scale
            current[side] = value.astype(jnp.bfloat16)
            factor[side] = ((jnp.where(diagonal, order + 1.0, 0.0) - value) * inverse_order).astype(
                jnp.bfloat16
            )

        product(gradient, gradient, dims, start_root)

    @pl.loop(0, 2)
    def _(side):
        def keep(ref):
            def finish(tile):
                ref[...] = tile.astype(jnp.bfloat16)

            return finish

        def next_factor(tile):
            second[...] = (
                (jnp.where(on_diagonal(), order + 1.0, 0.0) - tile) * inverse_order
            ).astype(jnp.bfloat16)

        product(factor.at[side], factor.at[side], NORMAL, keep(square.at[0]))

        @pl.when(quartic == 1)
        def _():
            product(square.at[0], square.at[0], NORMAL, keep(square.at[1]))

        product(square.at[quartic], current.at[side], NORMAL, next_factor)
        product(factor.at[side], second, NORMAL, keep(roots.at[side]))

    if with_update:
        half = lax.dot_general(roots[0], gradient[...], NORMAL, preferred_element_type=jnp.float32)
        second[...] = half.astype(jnp.bfloat16)
        whole = lax.dot_general(second[...], roots[1], NORMAL, preferred_element_type=jnp.float32)
        rounded = whole.astype(jnp.bfloat16)
        update[...] = rounded
        square_sum[...] = fold(rounded.astype(jnp.float32))


def run_block(with_update, inputs, act_at, grad_at, filled, exponent, damping, gate, place=(0, 1), held=None):
    unread = ([] if held is None else [held]) + list(gate)
    tokens = inputs.shape[0]
    ints = jnp.stack([act_at, grad_at, filled.astype(jnp.int32), exponent])
    one = pltpu.VMEM((BLK, BLK), jnp.bfloat16)
    two = pltpu.VMEM((2, BLK, BLK), jnp.bfloat16)
    scratch = [one, two, two, one, two]
    if with_update:
        scratch.append(two)
        shapes = (
            jax.ShapeDtypeStruct((BLK, BLK), jnp.bfloat16),
            jax.ShapeDtypeStruct((8, BLK), jnp.float32),
        )
        specs = (
            pl.BlockSpec((BLK, BLK), lambda i, a, b: (0, 0)),
            pl.BlockSpec((8, BLK), lambda i, a, b: (0, 0)),
        )
    else:
        position, count = place
        shapes = jax.ShapeDtypeStruct((count, 2, BLK, BLK), jnp.bfloat16)
        specs = pl.BlockSpec((1, 2, BLK, BLK), lambda i, a, b: (position, 0, 0, 0))
    products = 13 if with_update else 11
    return pl.pallas_call(
        functools.partial(block_kernel, with_update, len(unread)),
        out_shape=shapes,
        grid_spec=pltpu.PrefetchScalarGridSpec(
            num_scalar_prefetch=2,
            grid=(1,),
            in_specs=[
                pl.BlockSpec((tokens, BLK), lambda i, a, b: (0, a[0])),
                pl.BlockSpec((tokens, BLK), lambda i, a, b: (0, a[1])),
            ]
            + [pl.BlockSpec(memory_space=pl.ANY)] * len(unread),
            out_specs=specs,
            scratch_shapes=scratch,
        ),
        compiler_params=pltpu.CompilerParams(vmem_limit_bytes=52 * 1024 * 1024),
        cost_estimate=pl.CostEstimate(
            flops=products * 2 * BLK**3, bytes_accessed=8 * BLK**2, transcendentals=0
        ),
        name="block_update" if with_update else "block_roots",
        input_output_aliases={} if held is None else {4: 0},
    )(ints, damping[None], inputs, inputs, *unread)


def unfilled(shape, after):
    return pl.pallas_call(
        lambda after_ref, out_ref: None,
        out_shape=jax.ShapeDtypeStruct(shape, jnp.bfloat16),
        in_specs=[pl.BlockSpec(memory_space=pl.ANY)],
        out_specs=pl.BlockSpec(memory_space=pl.ANY),
        name="unfilled",
    )(after)


def share_kernel(owners, halves, own, out, places, send_sems, recv_sems):
    count = owners * halves
    me = lax.axis_index("dp") * halves + lax.axis_index("mp")

    def peer(offset):
        other = lax.rem(me + offset, count)
        return {"dp": other // halves, "mp": lax.rem(other, halves)}

    barrier = pltpu.get_barrier_semaphore()
    for offset in range(1, count):
        pl.semaphore_signal(barrier, inc=1, device_id=peer(offset), device_id_type=pl.DeviceIdType.MESH)
    pl.semaphore_wait(barrier, count - 1)
    copies = []
    for offset in range(1, count):
        copies.append(
            pltpu.make_async_remote_copy(
                src_ref=own,
                dst_ref=places.at[me],
                send_sem=send_sems.at[offset],
                recv_sem=recv_sems.at[offset],
                device_id=peer(offset),
                device_id_type=pl.DeviceIdType.MESH,
            )
        )
    for copy in copies:
        copy.start()
    places[me] = own[...]
    for copy in copies:
        copy.wait()
    total = places[0]
    for index in range(1, count):
        total = total + places[index]
    out[...] = total


def shared_sum(own, owners, halves):
    count = owners * halves
    return pl.pallas_call(
        functools.partial(share_kernel, owners, halves),
        out_shape=jax.ShapeDtypeStruct(own.shape, own.dtype),
        in_specs=[pl.BlockSpec(memory_space=pltpu.VMEM)],
        out_specs=pl.BlockSpec(memory_space=pltpu.VMEM),
        scratch_shapes=[
            pltpu.VMEM((count,) + own.shape, own.dtype),
            pltpu.SemaphoreType.DMA((count,)),
            pltpu.SemaphoreType.DMA((count,)),
        ],
        compiler_params=pltpu.CompilerParams(collective_id=0, has_side_effects=True),
        cost_estimate=pl.CostEstimate(flops=10**9, bytes_accessed=10**6, transcendentals=0),
        name="shared_sum",
    )(own)


def ring_order(size):
    return list(range(0, size, 2)) + list(range(size - 1 - size % 2, 0, -2))


def two_way_ring(own, size, place, base=0):
    order = ring_order(size)
    forward = [(order[i], order[(i + 1) % size]) for i in range(size)]
    backward = [(b, a) for a, b in forward]
    order_array = jnp.array(order, jnp.int32)
    seat_array = jnp.array([order.index(i) for i in range(size)], jnp.int32)
    seat = seat_array[lax.axis_index("dp")]
    rows = own.shape[0]
    whole = (size - 1) // 2
    ahead = behind = own
    arrived = []
    for step in range(1, whole + 1):
        ahead = lax.ppermute(ahead, "dp", forward)
        behind = lax.ppermute(behind, "dp", backward)
        arrived.append((ahead, behind))
        place(order_array[(seat - step) % size], base, ahead)
        place(order_array[(seat + step) % size], base, behind)
    if size % 2 == 0:
        across = order_array[(seat + size // 2) % size]
        place(across, base, lax.ppermute(ahead[: rows // 2], "dp", forward))
        place(across, base + rows // 2, lax.ppermute(behind[rows // 2 :], "dp", backward))
    return arrived


def on_device(activations, out_grads, slot_table, exponent_index, damping_index):
    tok_count = activations.shape[0]
    row_blocks = activations.shape[1] // BLK
    half_width = out_grads.shape[1]
    col_blocks = half_width // BLK
    half_blocks = row_blocks * col_blocks
    slot_count = slot_table.shape[1]
    owners = lax.axis_size("dp")
    halves = lax.axis_size("mp")
    per_owner = slot_count // owners
    me = lax.axis_index("dp")
    shared = min(owners, half_blocks)

    half_id = lax.axis_index("mp")
    act_parts = row_blocks // halves
    act_width = act_parts * BLK
    mine = lax.dynamic_slice(activations, (0, half_id * act_width), (tok_count, act_width))
    theirs = lax.dynamic_slice(activations, (0, (1 - half_id) * act_width), (tok_count, act_width))
    own = jnp.concatenate([mine, out_grads], axis=1)
    gathered = [unfilled((owners * tok_count, activations.shape[1] + half_width), own)]

    def store_input(source, offset, piece, other):
        at = source * tok_count + offset
        gathered[0] = lax.dynamic_update_slice(gathered[0], piece, (at, 0))
        gathered[0] = lax.dynamic_update_slice(gathered[0], other, (at, act_width + half_width))

    def place_input(source, offset, piece):
        other = lax.ppermute(piece[:, :act_width], "mp", [(0, 1), (1, 0)])
        store_input(source, offset, piece, other)

    store_input(me, 0, own, theirs)
    two_way_ring(own, owners, place_input)
    inputs = gathered[0]

    table = slot_table[0]
    exponents = exponent_index[0]
    picks = damping_index[0]
    dampings = jnp.sum(
        jnp.where(
            picks[:, None] == jnp.arange(len(DAMPINGS), dtype=jnp.int32)[None, :],
            jnp.asarray(DAMPINGS, jnp.float32)[None, :],
            0.0,
        ),
        axis=1,
    )

    def columns(block_id):
        row_id = block_id // col_blocks
        part = row_id // act_parts
        within = row_id % act_parts
        act_at = jnp.where(part == half_id, within, act_parts + col_blocks + within)
        return act_at, act_parts + block_id % col_blocks

    def block(block_id, gate=()):
        slot = table[block_id]
        act_at, grad_at = columns(block_id)
        return run_block(
            True, inputs, act_at, grad_at, jnp.int32(1), exponents[slot], dampings[slot], gate
        )

    first, first_sum = block((me % shared).astype(jnp.int32))
    lanes = jnp.where(me < shared, first_sum[:, :128], 0.0)
    for lane in range(128, BLK, 128):
        lanes = lanes + jnp.where(me < shared, first_sum[:, lane : lane + 128], 0.0)
    shared_total, first = lax.optimization_barrier((shared_sum(lanes, owners, halves), first))
    total_sq = jnp.sum(shared_total)

    waiting = []
    arrived = []
    for base in (0, BLK // 2):
        arrived.append(
            two_way_ring(
                first[base : base + BLK // 2], owners, lambda *piece: waiting.append(piece), base
            )
        )
    gates = [(), arrived[0][:1], arrived[1][:1], arrived[0][1:2] + arrived[1][1:2]]
    gates = [[piece for pair in gate for piece in pair] for gate in gates]
    extras = []
    extra_total = jnp.float32(0.0)
    for index in range(shared, half_blocks):
        gate = gates.pop(0) if len(gates) > 2 else ()
        extra, extra_sum = block(jnp.int32(index), gate)
        extras.append(extra)
        extra_total = extra_total + jnp.sum(extra_sum)
    if extras:
        held = jnp.full((8, 128), extra_total, jnp.float32)
        total_sq = total_sq + (extra_total + lax.ppermute(held, "mp", [(0, 1), (1, 0)])[0, 0])
    rescale = lax.rsqrt(total_sq / (row_blocks * BLK * half_width * halves) + 1.0)

    roots = None
    for position in range(per_owner):
        slot = me * per_owner + position
        matches = table[:half_blocks] == slot
        block_id = jnp.sum(jnp.where(matches, jnp.arange(half_blocks, dtype=jnp.int32), 0))
        act_at, grad_at = columns(block_id)
        roots = run_block(
            False, inputs, act_at, grad_at, jnp.any(matches), exponents[slot], dampings[slot],
            gates.pop(0) if gates else (), (position, per_owner), roots,
        )

    canvas = [unfilled((row_blocks * BLK, half_width), first)]

    def place_block(source, offset, piece):
        scaled = (piece.astype(jnp.float32) * rescale).astype(jnp.bfloat16)
        at = ((source // col_blocks) * BLK + offset, (source % col_blocks) * BLK)
        if shared < owners:
            before = lax.dynamic_slice(canvas[0], at, scaled.shape)
            scaled = jnp.where(source < shared, scaled, before)
        canvas[0] = lax.dynamic_update_slice(canvas[0], scaled, at)

    for position, extra in enumerate(extras):
        place_block(jnp.int32(shared + position), 0, extra)
    place_block(me, 0, first)
    for source, offset, piece in waiting:
        place_block(source, offset, piece)
    return (canvas[0], roots[None])


def solution(mesh):
    placed = (
        P(("member", "dp"), None),
        P(("member", "dp"), "mp"),
        P(("member", "mp"), None),
        P(("member", "mp"), None),
        P(("member", "mp"), None),
    )
    return jax.shard_map(
        on_device,
        mesh=mesh,
        in_specs=placed,
        out_specs=(P("member", "mp"), P(("member", "mp"), "dp", None, None, None)),
        check_vma=False,
    )
```

```python
import functools

import jax
import jax.numpy as jnp
from jax import lax
from jax.experimental import pallas as pl
from jax.experimental.pallas import tpu as pltpu
from jax.sharding import PartitionSpec as P

BLK = 1024

ROOT_ORDERS = (2.0, 4.0)
DAMPINGS = (0.03, 0.1, 0.3, 1.0)


NORMAL = (((1,), (0,)), ((), ()))
LEFT_T = (((0,), (0,)), ((), ()))
RIGHT_T = (((1,), (1,)), ((), ()))


def product(lhs, rhs, dims, finish):
    finish(lax.dot_general(lhs[...], rhs[...], dims, preferred_element_type=jnp.float32))


def on_diagonal():
    row = lax.broadcasted_iota(jnp.int32, (BLK, BLK), 0)
    return row == lax.broadcasted_iota(jnp.int32, (BLK, BLK), 1)


def fold(values):
    return jnp.sum((values * values).reshape(BLK // 8, 8, BLK), axis=0)


def block_kernel(with_update, unread, ints, floats, act, grad, *refs):
    refs = refs[unread:]
    if with_update:
        update, square_sum, gradient, current, factor, second, square, roots = refs
    else:
        roots_out, gradient, current, factor, second, square = refs
        roots = roots_out.at[0]
    filled = ints[2]
    quartic = ints[3]
    damping = floats[0]
    order = jnp.where(quartic == 1, 4.0, 2.0)
    inverse_order = jnp.where(quartic == 1, 0.25, 0.5)

    tile = lax.dot_general(act[...], grad[...], LEFT_T, preferred_element_type=jnp.float32)
    rounded = jnp.where(filled == 1, tile, 0.0).astype(jnp.bfloat16)
    gradient[...] = rounded
    trace = jnp.sum(fold(rounded.astype(jnp.float32)))
    shift = damping * (trace / BLK + 1.0)
    scale = BLK / (2.0 * (trace + BLK * shift))

    for side, dims in ((0, RIGHT_T), (1, LEFT_T)):

        def start_root(tile):
            diagonal = on_diagonal()
            value = (tile + jnp.where(diagonal, shift, 0.0)) * scale
            current[side] = value.astype(jnp.bfloat16)
            factor[side] = ((jnp.where(diagonal, order + 1.0, 0.0) - value) * inverse_order).astype(
                jnp.bfloat16
            )

        product(gradient, gradient, dims, start_root)

    @pl.loop(0, 2)
    def _(side):
        def keep(ref):
            def finish(tile):
                ref[...] = tile.astype(jnp.bfloat16)

            return finish

        def next_factor(tile):
            second[...] = (
                (jnp.where(on_diagonal(), order + 1.0, 0.0) - tile) * inverse_order
            ).astype(jnp.bfloat16)

        product(factor.at[side], factor.at[side], NORMAL, keep(square.at[0]))

        @pl.when(quartic == 1)
        def _():
            product(square.at[0], square.at[0], NORMAL, keep(square.at[1]))

        product(square.at[quartic], current.at[side], NORMAL, next_factor)
        product(factor.at[side], second, NORMAL, keep(roots.at[side]))

    if with_update:
        half = lax.dot_general(roots[0], gradient[...], NORMAL, preferred_element_type=jnp.float32)
        second[...] = half.astype(jnp.bfloat16)
        whole = lax.dot_general(second[...], roots[1], NORMAL, preferred_element_type=jnp.float32)
        rounded = whole.astype(jnp.bfloat16)
        update[...] = rounded
        square_sum[...] = fold(rounded.astype(jnp.float32))


def run_block(with_update, inputs, act_at, grad_at, filled, exponent, damping, gate, place=(0, 1), held=None):
    unread = ([] if held is None else [held]) + list(gate)
    tokens = inputs.shape[0]
    ints = jnp.stack([act_at, grad_at, filled.astype(jnp.int32), exponent])
    one = pltpu.VMEM((BLK, BLK), jnp.bfloat16)
    two = pltpu.VMEM((2, BLK, BLK), jnp.bfloat16)
    scratch = [one, two, two, one, two]
    if with_update:
        scratch.append(two)
        shapes = (
            jax.ShapeDtypeStruct((BLK, BLK), jnp.bfloat16),
            jax.ShapeDtypeStruct((8, BLK), jnp.float32),
        )
        specs = (
            pl.BlockSpec((BLK, BLK), lambda i, a, b: (0, 0)),
            pl.BlockSpec((8, BLK), lambda i, a, b: (0, 0)),
        )
    else:
        position, count = place
        shapes = jax.ShapeDtypeStruct((count, 2, BLK, BLK), jnp.bfloat16)
        specs = pl.BlockSpec((1, 2, BLK, BLK), lambda i, a, b: (position, 0, 0, 0))
    products = 13 if with_update else 11
    return pl.pallas_call(
        functools.partial(block_kernel, with_update, len(unread)),
        out_shape=shapes,
        grid_spec=pltpu.PrefetchScalarGridSpec(
            num_scalar_prefetch=2,
            grid=(1,),
            in_specs=[
                pl.BlockSpec((tokens, BLK), lambda i, a, b: (0, a[0])),
                pl.BlockSpec((tokens, BLK), lambda i, a, b: (0, a[1])),
            ]
            + [pl.BlockSpec(memory_space=pl.ANY)] * len(unread),
            out_specs=specs,
            scratch_shapes=scratch,
        ),
        compiler_params=pltpu.CompilerParams(vmem_limit_bytes=52 * 1024 * 1024),
        cost_estimate=pl.CostEstimate(
            flops=products * BLK**2, bytes_accessed=8 * BLK**2, transcendentals=0
        ),
        name="block_update" if with_update else "block_roots",
        input_output_aliases={} if held is None else {4: 0},
    )(ints, damping[None], inputs, inputs, *unread)


def unfilled(shape, after):
    return pl.pallas_call(
        lambda after_ref, out_ref: None,
        out_shape=jax.ShapeDtypeStruct(shape, jnp.bfloat16),
        in_specs=[pl.BlockSpec(memory_space=pl.ANY)],
        out_specs=pl.BlockSpec(memory_space=pl.ANY),
        name="unfilled",
    )(after)


def share_kernel(owners, halves, own, out, places, send_sems, recv_sems):
    count = owners * halves
    me = lax.axis_index("dp") * halves + lax.axis_index("mp")

    def peer(offset):
        other = lax.rem(me + offset, count)
        return {"dp": other // halves, "mp": lax.rem(other, halves)}

    barrier = pltpu.get_barrier_semaphore()
    for offset in range(1, count):
        pl.semaphore_signal(barrier, inc=1, device_id=peer(offset), device_id_type=pl.DeviceIdType.MESH)
    pl.semaphore_wait(barrier, count - 1)
    copies = []
    for offset in range(1, count):
        copies.append(
            pltpu.make_async_remote_copy(
                src_ref=own,
                dst_ref=places.at[me],
                send_sem=send_sems.at[offset],
                recv_sem=recv_sems.at[offset],
                device_id=peer(offset),
                device_id_type=pl.DeviceIdType.MESH,
            )
        )
    for copy in copies:
        copy.start()
    places[me] = own[...]
    for copy in copies:
        copy.wait()
    total = places[0]
    for index in range(1, count):
        total = total + places[index]
    out[...] = total


def shared_sum(own, owners, halves):
    count = owners * halves
    return pl.pallas_call(
        functools.partial(share_kernel, owners, halves),
        out_shape=jax.ShapeDtypeStruct(own.shape, own.dtype),
        in_specs=[pl.BlockSpec(memory_space=pltpu.VMEM)],
        out_specs=pl.BlockSpec(memory_space=pltpu.VMEM),
        scratch_shapes=[
            pltpu.VMEM((count,) + own.shape, own.dtype),
            pltpu.SemaphoreType.DMA((count,)),
            pltpu.SemaphoreType.DMA((count,)),
        ],
        compiler_params=pltpu.CompilerParams(collective_id=0, has_side_effects=True),
        cost_estimate=pl.CostEstimate(flops=10**6, bytes_accessed=10**6, transcendentals=0),
        name="shared_sum",
    )(own)


def ring_order(size):
    return list(range(0, size, 2)) + list(range(size - 1 - size % 2, 0, -2))


def two_way_ring(own, size, place, base=0):
    order = ring_order(size)
    forward = [(order[i], order[(i + 1) % size]) for i in range(size)]
    backward = [(b, a) for a, b in forward]
    order_array = jnp.array(order, jnp.int32)
    seat_array = jnp.array([order.index(i) for i in range(size)], jnp.int32)
    seat = seat_array[lax.axis_index("dp")]
    rows = own.shape[0]
    whole = (size - 1) // 2
    ahead = behind = own
    arrived = []
    for step in range(1, whole + 1):
        ahead = lax.ppermute(ahead, "dp", forward)
        behind = lax.ppermute(behind, "dp", backward)
        arrived.append((ahead, behind))
        place(order_array[(seat - step) % size], base, ahead)
        place(order_array[(seat + step) % size], base, behind)
    if size % 2 == 0:
        across = order_array[(seat + size // 2) % size]
        place(across, base, lax.ppermute(ahead[: rows // 2], "dp", forward))
        place(across, base + rows // 2, lax.ppermute(behind[rows // 2 :], "dp", backward))
    return arrived


def on_device(activations, out_grads, slot_table, exponent_index, damping_index):
    tok_count = activations.shape[0]
    row_blocks = activations.shape[1] // BLK
    half_width = out_grads.shape[1]
    col_blocks = half_width // BLK
    half_blocks = row_blocks * col_blocks
    slot_count = slot_table.shape[1]
    owners = lax.axis_size("dp")
    halves = lax.axis_size("mp")
    per_owner = slot_count // owners
    me = lax.axis_index("dp")
    shared = min(owners, half_blocks)

    half_id = lax.axis_index("mp")
    act_parts = row_blocks // halves
    act_width = act_parts * BLK
    mine = lax.dynamic_slice(activations, (0, half_id * act_width), (tok_count, act_width))
    theirs = lax.dynamic_slice(activations, (0, (1 - half_id) * act_width), (tok_count, act_width))
    own = jnp.concatenate([mine, out_grads], axis=1)
    gathered = [unfilled((owners * tok_count, activations.shape[1] + half_width), own)]

    def store_input(source, offset, piece, other):
        at = source * tok_count + offset
        gathered[0] = lax.dynamic_update_slice(gathered[0], piece, (at, 0))
        gathered[0] = lax.dynamic_update_slice(gathered[0], other, (at, act_width + half_width))

    def place_input(source, offset, piece):
        other = lax.ppermute(piece[:, :act_width], "mp", [(0, 1), (1, 0)])
        store_input(source, offset, piece, other)

    store_input(me, 0, own, theirs)
    two_way_ring(own, owners, place_input)
    inputs = gathered[0]

    table = slot_table[0]
    exponents = exponent_index[0]
    picks = damping_index[0]
    dampings = jnp.sum(
        jnp.where(
            picks[:, None] == jnp.arange(len(DAMPINGS), dtype=jnp.int32)[None, :],
            jnp.asarray(DAMPINGS, jnp.float32)[None, :],
            0.0,
        ),
        axis=1,
    )

    def columns(block_id):
        row_id = block_id // col_blocks
        part = row_id // act_parts
        within = row_id % act_parts
        act_at = jnp.where(part == half_id, within, act_parts + col_blocks + within)
        return act_at, act_parts + block_id % col_blocks

    def block(block_id, gate=()):
        slot = table[block_id]
        act_at, grad_at = columns(block_id)
        return run_block(
            True, inputs, act_at, grad_at, jnp.int32(1), exponents[slot], dampings[slot], gate
        )

    first, first_sum = block((me % shared).astype(jnp.int32))
    lanes = jnp.where(me < shared, first_sum[:, :128], 0.0)
    for lane in range(128, BLK, 128):
        lanes = lanes + jnp.where(me < shared, first_sum[:, lane : lane + 128], 0.0)
    shared_total, first = lax.optimization_barrier((shared_sum(lanes, owners, halves), first))
    total_sq = jnp.sum(shared_total)

    waiting = []
    arrived = []
    for base in (0, BLK // 2):
        arrived.append(
            two_way_ring(
                first[base : base + BLK // 2], owners, lambda *piece: waiting.append(piece), base
            )
        )
    gates = [(), arrived[0][1:2], arrived[1][1:2], arrived[0][2:3] + arrived[1][2:3]]
    gates = [[piece for pair in gate for piece in pair] for gate in gates]
    extras = []
    extra_total = jnp.float32(0.0)
    for index in range(shared, half_blocks):
        gate = gates.pop(0) if len(gates) > 2 else ()
        extra, extra_sum = block(jnp.int32(index), gate)
        extras.append(extra)
        extra_total = extra_total + jnp.sum(extra_sum)
    if extras:
        held = jnp.full((8, 128), extra_total, jnp.float32)
        total_sq = total_sq + (extra_total + lax.ppermute(held, "mp", [(0, 1), (1, 0)])[0, 0])
    rescale = lax.rsqrt(total_sq / (row_blocks * BLK * half_width * halves) + 1.0)

    roots = None
    for position in range(per_owner):
        slot = me * per_owner + position
        matches = table[:half_blocks] == slot
        block_id = jnp.sum(jnp.where(matches, jnp.arange(half_blocks, dtype=jnp.int32), 0))
        act_at, grad_at = columns(block_id)
        roots = run_block(
            False, inputs, act_at, grad_at, jnp.any(matches), exponents[slot], dampings[slot],
            gates.pop(0) if gates else (), (position, per_owner), roots,
        )

    canvas = [unfilled((row_blocks * BLK, half_width), first)]

    def place_block(source, offset, piece):
        scaled = (piece.astype(jnp.float32) * rescale).astype(jnp.bfloat16)
        at = ((source // col_blocks) * BLK + offset, (source % col_blocks) * BLK)
        if shared < owners:
            before = lax.dynamic_slice(canvas[0], at, scaled.shape)
            scaled = jnp.where(source < shared, scaled, before)
        canvas[0] = lax.dynamic_update_slice(canvas[0], scaled, at)

    for position, extra in enumerate(extras):
        place_block(jnp.int32(shared + position), 0, extra)
    place_block(me, 0, first)
    for source, offset, piece in waiting:
        place_block(source, offset, piece)
    return (canvas[0], roots[None])


def solution(mesh):
    placed = (
        P(("member", "dp"), None),
        P(("member", "dp"), "mp"),
        P(("member", "mp"), None),
        P(("member", "mp"), None),
        P(("member", "mp"), None),
    )
    return jax.shard_map(
        on_device,
        mesh=mesh,
        in_specs=placed,
        out_specs=(P("member", "mp"), P(("member", "mp"), "dp", None, None, None)),
        check_vma=False,
    )
```
